256 devices in a mesh: row: 32 (over x_hi, z, core), ga: 8 (over x_lo, y).
Axes of the slice: x: 4 (x_hi: 2, x_lo: 2; x = x_hi * 2 + x_lo), y: 4, z: 8, core: 2. Of those that a mesh axis runs over, the one named last changes fastest.
Arguments:
- pair_dens: bfloat16 [32, 256, 4096], P('row', None, 'ga'), may hold values from -0.41992188 to 0.41992188
- cond_dens: bfloat16 [32, 1024, 4096], P('row', None, 'ga'), may hold values from -0.41992188 to 0.41992188
- val_dens: bfloat16 [32, 64, 4096], P(None, None, 'row'), may hold values from -0.41992188 to 0.41992188
- screened: bfloat16 [8, 4096, 4096], P(None, 'ga', 'row'), may hold values from -1 to 6, as said below
- coulomb: bfloat16 [4096], P('ga'), may hold values from 0.29882812 to 10
- pair_list: int32 [32, 256], replicated, may hold values from 0 to 255, each once within a row
- counts: int32 [32], replicated, may hold values from 10 to 256
- q_index: int32 [32], replicated, may hold values from 0 to 7
- column_k: int32 [1], replicated, may hold values from 0 to 31
Outputs:
- kernel: bfloat16 [8192, 256], P('row', 'ga')
The draws below stay inside these ranges and needn't reach their ends.
Inputs may be any that keep to these rules, and one draw needn't show every extreme that they name: `screened`: each diagonal entry exceeds the sum of the magnitudes of the others in its row divided by the square root of 4096 times four.
All inputs are finite; a program needn't handle non-finite values.
Results may differ from the reference program's by a relative error of at most 0.0042.
Values may be sent and summed in bfloat16 or wider, within the bound.
A program may use at most 64 MiB of HBM per device.

```python
import math
import jax
import jax.numpy as jnp
from jax import lax

NV = 8
NC = 32
G = 4096
NQ = 8
PMAX = 256
VV = 64
NK = 32


def draw_screened(key, part):
    first = jax.random.fold_in(key, 11)
    second = jax.random.fold_in(key, 12)
    noise = jnp.clip(jax.random.normal(first, (NQ, G, G)), -4.0, 4.0)
    diag = jnp.exp(jax.random.uniform(second, (NQ, G), minval=0.0, maxval=math.log(5.0)))
    same = jnp.arange(G)[:, None] == jnp.arange(G)[None, :]
    return (noise / math.sqrt(G) + jnp.where(same[None, :, :], diag[:, :, None], 0.0)).astype(jnp.bfloat16)


def place_ends(result, own_key, smallest, top_value):
    dims = result.shape
    index_at = [jax.random.randint(jax.random.fold_in(own_key, axis), (), 0, dims[axis]) for axis in range(len(dims))]
    result = result.at[tuple(index_at)].set(smallest)
    longest = dims.index(max(dims))
    index_at[longest] = (index_at[longest] + 1) % dims[longest]
    return result.at[tuple(index_at)].set(top_value)


def shard_levels(stream_key, shape, shards, low, largest):
    def one(dim, shards_of):
        draws = jax.random.uniform(jax.random.fold_in(jax.random.fold_in(stream_key, 6), dim), (shards_of,), jnp.float32, low / len(shards), largest / len(shards))
        return jnp.repeat(jnp.exp(draws), shape[dim] // shards_of).reshape((-1,) + (1,) * (len(shape) - dim - 1))

    loudness = one(*shards[0])
    for cut in shards[1:]:
        loudness = loudness * one(*cut)
    return loudness


def gaussian(rng, extent, width, limit, pieces=(), kind=jnp.bfloat16):
    result = width * jax.random.normal(rng, extent, jnp.float32)
    if pieces:
        result = result * shard_levels(rng, extent, pieces, -0.22, 0.18)
    return jnp.clip(result, -limit, limit).astype(kind)


def setup_inputs(seed: int = 0) -> dict:
    keys = jax.random.split(jax.random.key(seed), 10)
    pair_dens = gaussian(keys[0], (NK, PMAX, G), 0.07, 0.41992188, ((0, 32), (2, 8)))
    cond_dens = gaussian(keys[1], (NK, NC * NC, G), 0.07, 0.41992188, ((0, 32), (2, 8)))
    val_dens = gaussian(keys[2], (NK, VV, G), 0.07, 0.41992188, ((2, 32),))
    screened = draw_screened(jax.random.fold_in(keys[9], 71), 0)
    coulomb = jnp.clip(jnp.exp(math.log(10.0) - 3.5104718 * jax.random.uniform(keys[4], (G,), jnp.float32) ** shard_levels(keys[4], (G,), ((0, 8),), -0.2, 0.2)), 0.29882812, 10.0).astype(jnp.bfloat16)
    pair_list = jax.vmap(lambda own: jax.random.permutation(own, PMAX))(jax.random.split(keys[5], NK)).reshape((NK, PMAX)).astype(jnp.int32)
    counts = place_ends(jax.random.randint(keys[6], (NK,), max(2, NV * NC // 25), min(401, NV * NC + 1)), jax.random.fold_in(keys[6], 1), max(2, NV * NC // 25), (min(401, NV * NC + 1)) - 1).astype(jnp.int32)
    q_index = place_ends(jax.random.randint(keys[7], (NK,), 0, NQ), jax.random.fold_in(keys[7], 1), 0, NQ - 1).astype(jnp.int32)
    column_k = jax.random.randint(keys[8], (1,), 0, NK).astype(jnp.int32)
    return {"pair_dens": pair_dens, "cond_dens": cond_dens, "val_dens": val_dens, "screened": screened, "coulomb": coulomb, "pair_list": pair_list, "counts": counts, "q_index": q_index, "column_k": column_k}


def reference(pair_dens, cond_dens, val_dens, screened, coulomb, pair_list, counts, q_index, column_k):
    column = column_k[0]
    col_pairs = pair_list[column]
    col = jnp.take(pair_dens[column], col_pairs, axis=0)
    col_count = counts[column]
    slots = jnp.arange(NV * NC, dtype=jnp.int32)
    col_mask = (slots < col_count).astype(jnp.float32)

    def one_point(index):
        pairs = pair_list[index]
        rows = jnp.take(pair_dens[index], pairs, axis=0)
        weighted = (rows.astype(jnp.float32) * coulomb.astype(jnp.float32)[None, :]).astype(jnp.bfloat16)
        exch = jnp.dot(weighted, col.T, preferred_element_type=jnp.float32)
        wmat = screened[q_index[index]]
        screened_val = jnp.dot(val_dens[index], wmat.T, preferred_element_type=jnp.float32).astype(jnp.bfloat16)
        direct_full = jnp.dot(cond_dens[index], screened_val.T, preferred_element_type=jnp.float32)
        arranged = direct_full.reshape(NC, NC, NV, NV).transpose(2, 0, 3, 1).reshape(NV * NC, NV * NC)
        direct = jnp.take(jnp.take(arranged, pairs, axis=0), col_pairs, axis=1)
        row_mask = (slots < counts[index]).astype(jnp.float32)
        block = (2.0 * exch - direct) * row_mask[:, None] * col_mask[None, :]
        return block.astype(jnp.bfloat16)

    blocks = lax.map(one_point, jnp.arange(pair_dens.shape[0], dtype=jnp.int32))
    return blocks.reshape(pair_dens.shape[0] * NV * NC, NV * NC)
```

```python
import jax
import jax.numpy as jnp
from jax import lax
from jax.experimental import pallas as pl
from jax.experimental.pallas import tpu as pltpu
from jax.sharding import PartitionSpec as P

NV = 8
NC = 32
F32 = jnp.float32
BF16 = jnp.bfloat16
MESH = pl.DeviceIdType.MESH

ORDER = (4, 3, 5, 2, 6, 1, 7, 0)


def dot_t(a, b):
    return lax.dot_general(a, b, (((1,), (1,)), ((), ())), preferred_element_type=F32)


def dot_l(a, b):
    return lax.dot_general(a, b, (((0,), (0,)), ((), ())), preferred_element_type=F32)


def one_hot(condition):
    return jnp.where(condition, 1.0, 0.0).astype(BF16)


def iota(shape, dim):
    return lax.broadcasted_iota(jnp.int32, shape, dim)


def kernel(
    counts, q_index, column_k, pairs, coulomb, pd_hbm, cond_hbm, val_hbm, scr_hbm, out_ref,
    pd, cond, val, scr, own, obuf, orecv, zsend, zrecv, xsend, xrecv, mine_sum,
    cgb, c0buf, cand, c1buf, colbuf, perm, wperm, pick, exch, gsend, grecv,
    load_sem, o_s, o_r, z_s, z_r, x_s, x_r, c0_s, c0_r, c1_s, c1_r, c2_s, c2_r, c3_s, c3_r, g_s, g_r,
):
    row = lax.axis_index("row")
    ga = lax.axis_index("ga")
    core = row % 2
    z = (row // 2) % 8
    h = row // 16
    sent = []

    def at(hh, zz, cc):
        return {"row": (hh * 8 + zz) * 2 + cc, "ga": ga}

    def send(src, dst, s, r, where):
        copy = pltpu.make_async_remote_copy(
            src_ref=src, dst_ref=dst, send_sem=s, recv_sem=r, device_id=where, device_id_type=MESH
        )
        copy.start()
        sent.append(copy)
        return copy

    partner = at(h, z, 1 - core)
    far = at(1 - h, z, core)
    chips = [(dh, dz) for dz in (4, 3, 5, 2, 6, 1, 7, 0) for dh in (1, 0) if (dh, dz) != (0, 0)]

    loads = [
        pltpu.make_async_copy(src, dst, load_sem.at[i])
        for i, (src, dst) in enumerate(
            ((pd_hbm.at[0], pd), (val_hbm, val), (scr_hbm, scr), (cond_hbm.at[0], cond))
        )
    ]
    for load in loads:
        load.start()

    barrier = pltpu.get_barrier_semaphore()
    peers = [partner] + [at((h + dh) % 2, (z + dz) % 8, core) for dh, dz in chips]
    peers += [{"row": row, "ga": (ga + d) % 8} for d in range(1, 8)]
    for peer in peers:
        pl.semaphore_signal(barrier, inc=1, device_id=peer, device_id_type=MESH)

    ck = column_k[0]
    root_h = ck // 16
    root_z = (ck // 2) % 8
    root_core = ck % 2
    cp = pairs[pl.ds(ck, 1), :]

    loads[0].wait()
    gather = one_hot(iota((256, 256), 0) == cp)
    cg = dot_l(gather, pd[...]).astype(BF16)
    for c in range(2):
        for s in range(2):
            cgb[c, s] = cg[c * 128 : c * 128 + 128, s * 256 : s * 256 + 256].reshape(8, 16, 256)

    loads[1].wait()
    loads[2].wait()

    def product(side, dz, cc):
        k = (((h + 1 - side) % 2) * 8 + (z + dz) % 8) * 2 + cc
        return dot_t(val[k], scr[q_index[k]])

    def others(dz):
        for side in range(2):
            obuf[dz, side] = product(side, dz, 1 - core).astype(BF16)

    o_copies = {}

    def send_others(dz):
        o_copies[dz] = send(obuf.at[dz], orecv.at[dz], o_s.at[dz], o_r.at[dz], partner)

    def mine(dz):
        o_copies[dz].wait_recv()
        for side in range(2):
            own[dz, side] = product(side, dz, core) + orecv[dz, side].astype(F32)

    z_copies = {}

    def half(w):
        return pl.ds(w * 32, 32)

    def z_send(d, side, slot, value):
        zsend[d, side, slot] = value.astype(BF16)
        z_copies[d, side, slot] = send(
            zsend.at[d, side, slot], zrecv.at[d, side, slot], z_s.at[d, side, slot], z_r.at[d, side, slot],
            at(h, (z + (1, 7)[d]) % 8, core),
        )

    def z_got(d, side, slot):
        z_copies[d, side, slot].wait_recv()
        return zrecv[d, side, slot].astype(F32)

    others(4)
    others(3)
    others(5)
    pl.semaphore_wait(barrier, len(peers))
    c0 = send(cgb.at[1 - core], c0buf, c0_s, c0_r, partner)
    for dz in (4, 3, 5):
        send_others(dz)
    for dz in ORDER[3:]:
        others(dz)
        send_others(dz)

    c0.wait_recv()
    cand[...] = jnp.where(root_core == core, cgb[core], c0buf[...])
    c1 = []
    for i, (dh, dz) in enumerate(chips):
        hh, zz = (h + dh) % 2, (z + dz) % 8
        c1.append(send(cand.at[hh, zz], c1buf.at[h, z], c1_s.at[i], c1_r.at[i], at(hh, zz, core)))
    c1buf[h, z] = cand[h, z]

    mine(4)
    for side in range(2):
        z_send(0, side, 0, own[4, side, half(0), :])
        z_send(1, side, 0, own[4, side, half(1), :])
    mine(3)
    for side in range(2):
        z_send(0, side, 1, own[3, side, half(1), :])
    mine(5)
    for side in range(2):
        z_send(1, side, 1, own[5, side, half(0), :])
    for dz in ORDER[3:]:
        mine(dz)

    def relay(slot):
        for side in range(2):
            for d in range(2):
                dz = (4 - (slot + 1) // 2) * (1, 7)[d] % 8
                first_half = slot % 2 == 0
                w = d if first_half else 1 - d
                z_send(d, side, slot, own[dz, side, half(w), :] + z_got(d, side, slot - 2))

    relay(2)
    relay(3)

    wt = (pd[...].astype(F32) * coulomb[...].astype(F32)).astype(BF16)
    r0, p0 = iota((256, 256), 0), iota((256, 256), 1)
    order = one_hot(p0 == (r0 % 8) * 32 + ((r0 // 8) % 8) * 4 + r0 // 64)
    wperm[...] = jnp.dot(order, wt, preferred_element_type=F32).astype(BF16)
    kp = pairs[pl.ds(row, 1), :]
    kc = kp % 32
    target = (kc % 4) * 64 + (kc // 4) * 8 + kp // 32
    perm[...] = jnp.transpose(
        jnp.where((r0 == target) & (p0 < counts[row]), 1.0, 0.0).astype(F32)
    ).astype(BF16)
    i0 = iota((128, 256), 0)
    for j in range(4):
        pick[j] = one_hot((i0 // 32 == j) & (i0 % 32 == cp % 32))

    relay(4)

    for copy in c1:
        copy.wait_recv()
    colbuf[h, core, z] = c1buf[root_h, root_z]
    c2 = []
    for i, (dh, dz) in enumerate(chips):
        mine_slot = colbuf.at[h, core, z]
        c2.append(send(mine_slot, mine_slot, c2_s.at[i], c2_r.at[i], at((h + dh) % 2, (z + dz) % 8, core)))

    relay(5)
    relay(6)

    x_copies = []
    for w in range(2):
        total = own[0, 0, half(w), :] + z_got(w, 0, 6) + z_got(1 - w, 0, 5)
        xsend[w] = total.astype(BF16)
        x_copies.append(send(xsend.at[w], xrecv.at[w], x_s.at[w], x_r.at[w], far))
    for w in range(2):
        mine_sum[half(w), :] = own[0, 1, half(w), :] + z_got(w, 1, 6) + z_got(1 - w, 1, 5)

    for copy in c2:
        copy.wait_recv()
    c3 = []
    for s in range(2):
        c3.append(send(colbuf.at[s, core], colbuf.at[s, core], c3_s.at[s], c3_r.at[s], partner))
    for copy in c3:
        copy.wait_recv()
    exch[...] = 2.0 * (
        dot_t(wperm[:, 0:256], colbuf[0].reshape(256, 256))
        + dot_t(wperm[:, 256:512], colbuf[1].reshape(256, 256))
    )

    loads[3].wait()
    for copy in x_copies:
        copy.wait_recv()
    sv = (mine_sum[...] + xrecv[...].reshape(64, 512).astype(F32)).astype(BF16)
    w0, w1 = iota((64, 64), 0), iota((64, 64), 1)
    swap = one_hot(w1 == (w0 % 8) * 8 + w0 // 8)
    sv = jnp.dot(swap, sv, preferred_element_type=F32).astype(BF16)
    dt = dot_t(sv, cond[...]).astype(BF16)
    dt = jnp.concatenate([dt[:, b * 128 : b * 128 + 128] for b in range(8)], axis=0)
    v_of = cp // 32
    parts = []
    for j in range(4):
        e = jnp.dot(dt, pick[j], preferred_element_type=F32).reshape(8, 8, 8, 256)
        total = jnp.where(v_of == 0, e[:, 0], 0.0)
        for v in range(1, 8):
            total = total + jnp.where(v_of == v, e[:, v], 0.0)
        parts.append(exch[j * 64 : j * 64 + 64, :] - total.reshape(64, 256))
    for d in range(8):
        piece = jnp.concatenate([p[:, d * 32 : d * 32 + 32] for p in parts], axis=1)
        gsend[d] = piece.astype(BF16)
    g_copies = []
    for d in range(1, 8):
        to = (ga + d) % 8
        g_copies.append(
            send(gsend.at[to], grecv.at[d - 1], g_s.at[d - 1], g_r.at[d - 1], {"row": row, "ga": to})
        )
    total = gsend[ga].astype(F32)
    for d, copy in enumerate(g_copies):
        copy.wait_recv()
        total = total + grecv[d].astype(F32)
    total = total.astype(BF16).astype(F32)
    stacked = jnp.concatenate(
        [total if j == 0 else pltpu.roll(total, 128 - 32 * j, 1) for j in range(4)], axis=0
    ).astype(BF16)
    result = jnp.dot(perm[...], stacked, preferred_element_type=F32)
    slot = ga * 32 + iota((256, 128), 1)
    result = jnp.where(slot < counts[ck], result, 0.0)
    out_ref[...] = result[:, 0:32].astype(BF16)
    for copy in sent:
        copy.wait_send()


def per_device(
    pair_dens, cond_dens, val_dens, screened, coulomb, pair_list, counts, q_index, column_k
):
    dma = pltpu.SemaphoreType.DMA
    smem = pl.BlockSpec(memory_space=pltpu.SMEM)
    vmem = pl.BlockSpec(memory_space=pltpu.VMEM)
    hbm = pl.BlockSpec(memory_space=pl.ANY)
    return pl.pallas_call(
        kernel,
        out_shape=jax.ShapeDtypeStruct((256, 32), BF16),
        in_specs=[smem, smem, smem, vmem, vmem, hbm, hbm, hbm, hbm],
        out_specs=vmem,
        scratch_shapes=[
            pltpu.VMEM((256, 512), BF16),
            pltpu.VMEM((1024, 512), BF16),
            pltpu.VMEM((32, 64, 128), BF16),
            pltpu.VMEM((8, 512, 128), BF16),
            pltpu.VMEM((8, 2, 64, 512), F32),
            pltpu.VMEM((8, 2, 64, 512), BF16),
            pltpu.VMEM((8, 2, 64, 512), BF16),
            pltpu.VMEM((2, 2, 7, 32, 512), BF16),
            pltpu.VMEM((2, 2, 7, 32, 512), BF16),
            pltpu.VMEM((2, 32, 512), BF16),
            pltpu.VMEM((2, 32, 512), BF16),
            pltpu.VMEM((64, 512), F32),
            pltpu.VMEM((2, 2, 8, 16, 256), BF16),
            pltpu.VMEM((2, 8, 16, 256), BF16),
            pltpu.VMEM((2, 8, 16, 256), BF16),
            pltpu.VMEM((2, 8, 16, 256), BF16),
            pltpu.VMEM((2, 2, 8, 16, 256), BF16),
            pltpu.VMEM((256, 256), BF16),
            pltpu.VMEM((256, 512), BF16),
            pltpu.VMEM((4, 128, 256), BF16),
            pltpu.VMEM((256, 256), F32),
            pltpu.VMEM((8, 64, 128), BF16),
            pltpu.VMEM((7, 64, 128), BF16),
            dma((4,)),
            dma((8,)), dma((8,)),
            dma((2, 2, 7)), dma((2, 2, 7)),
            dma((2,)), dma((2,)),
            dma, dma,
            dma((15,)), dma((15,)),
            dma((15,)), dma((15,)),
            dma((2,)), dma((2,)),
            dma((7,)), dma((7,)),
        ],
        compiler_params=pltpu.CompilerParams(
            collective_id=0, has_side_effects=True, vmem_limit_bytes=48 * 1024 * 1024
        ),
        name="bse_block",
    )(
        counts, q_index, column_k, pair_list, coulomb.reshape(1, -1),
        pair_dens, cond_dens, val_dens, screened,
    )


def solution(mesh):
    placed = (
        P("row", None, "ga"),
        P("row", None, "ga"),
        P(None, None, "row"),
        P(None, "ga", "row"),
        P("ga"),
        P(),
        P(),
        P(),
        P(),
    )
    return jax.shard_map(
        per_device, mesh=mesh, in_specs=placed, out_specs=P("row", "ga"), check_vma=False
    )
```

```python
import jax
import jax.numpy as jnp
from jax import lax
from jax.experimental import pallas as pl
from jax.experimental.pallas import tpu as pltpu
from jax.sharding import PartitionSpec as P

NV = 8
NC = 32
F32 = jnp.float32
BF16 = jnp.bfloat16
MESH = pl.DeviceIdType.MESH

ORDER = (4, 3, 5, 2, 6, 1, 7, 0)


def dot_t(a, b):
    return lax.dot_general(a, b, (((1,), (1,)), ((), ())), preferred_element_type=F32)


def dot_l(a, b):
    return lax.dot_general(a, b, (((0,), (0,)), ((), ())), preferred_element_type=F32)


def one_hot(condition):
    return jnp.where(condition, 1.0, 0.0).astype(BF16)


def iota(shape, dim):
    return lax.broadcasted_iota(jnp.int32, shape, dim)


def kernel(
    counts_hbm, q_hbm, column_hbm, pairs_hbm, coul_hbm, pd_hbm, cond_hbm, val_hbm, scr_hbm, out_ref,
    counts, q_index, column_k, pairs, coulomb, pd, cond, val, scr, own, obuf, orecv, zsend, zrecv, xb_from, xb_recv, xsend, xrecv, mine_sum,
    cgb, c0buf, cand, cxbuf, quarter, c1buf, colbuf, perm, wperm, pick, direct, gsend, grecv,
    load_sem, o_s, o_r, z_s, z_r, xb_s, xb_r, x_s, x_r, c0_s, c0_r, cx_s, cx_r, c1_s, c1_r, c2_s, c2_r, c3_s, c3_r, g_s, g_r, tokens,
):
    row = lax.axis_index("row")
    ga = lax.axis_index("ga")
    core = row % 2
    z = (row // 2) % 8
    h = row // 16
    sent = []

    def at(hh, zz, cc):
        return {"row": (hh * 8 + zz) * 2 + cc, "ga": ga}

    def send(src, dst, s, r, where):
        copy = pltpu.make_async_remote_copy(
            src_ref=src, dst_ref=dst, send_sem=s, recv_sem=r, device_id=where, device_id_type=MESH
        )
        copy.start()
        sent.append(copy)
        return copy

    partner = at(h, z, 1 - core)
    far = at(1 - h, z, core)
    chips = [(dh, dz) for dz in (4, 3, 5, 2, 6, 1, 7, 0) for dh in (1, 0) if (dh, dz) != (0, 0)]

    loads = [
        pltpu.make_async_copy(src, dst, load_sem.at[i])
        for i, (src, dst) in enumerate(
            (
                (column_hbm, column_k), (pairs_hbm, pairs), (q_hbm, q_index), (pd_hbm.at[0], pd),
                (val_hbm, val), (scr_hbm, scr), (cond_hbm.at[0], cond), (counts_hbm, counts), (coul_hbm, coulomb),
            )
        )
    ]
    for load in loads:
        load.start()

    barrier = pltpu.get_barrier_semaphore()
    near = [at(h, (z + d) % 8, core) for d in (1, 7, 2, 6)]
    near += [{"row": row, "ga": (ga // 4) * 4 + (ga + d) % 4} for d in (1, 3, 2)]
    near.append({"row": row, "ga": (ga + 4) % 8})
    for peer in near + [far, partner]:
        pl.semaphore_signal(barrier, inc=1, device_id=peer, device_id_type=MESH)

    loads[0].wait()
    loads[1].wait()
    ck = column_k[0]
    root_h = ck // 16
    root_z = (ck // 2) % 8
    root_core = ck % 2
    cp = pairs[pl.ds(ck, 1), :]

    loads[3].wait()
    gather = one_hot(iota((256, 256), 0) == cp)
    cg = dot_l(gather, pd[...]).astype(BF16)
    for c in range(2):
        for s in range(2):
            cgb[c, s] = cg[c * 128 : c * 128 + 128, s * 256 : s * 256 + 256].reshape(8, 16, 256)

    for load in (loads[2], loads[4], loads[5]):
        load.wait()

    def product(side, dz, cc):
        k = (((h + 1 - side) % 2) * 8 + (z + dz) % 8) * 2 + cc
        return dot_t(val[k], scr[q_index[k]])

    def others(dz):
        for side in range(2):
            obuf[dz, side] = product(side, dz, 1 - core).astype(BF16)

    o_copies = {}

    def send_others(dz):
        o_copies[dz] = send(obuf.at[dz], orecv.at[dz], o_s.at[dz], o_r.at[dz], partner)

    def mine(dz):
        o_copies[dz].wait_recv()
        for side in range(2):
            own[dz, side] = product(side, dz, core) + orecv[dz, side].astype(F32)

    z_copies = {}

    def part(unit, dz, q):
        if unit < 2:
            return own[dz, unit, pl.ds(q * 16, 16), :]
        return own[dz, 1, pl.ds(32 + q * 16, 16), :] + xb_recv[dz, pl.ds(q * 16, 16), :].astype(F32)

    def z_send(d, unit, slot, value):
        zsend[d, unit, slot] = value.astype(BF16)
        z_copies[d, unit, slot] = send(
            zsend.at[d, unit, slot], zrecv.at[d, unit, slot], z_s.at[d, unit, slot], z_r.at[d, unit, slot],
            at(h, (z + (1, 7)[d]) % 8, core),
        )

    def z_got(d, unit, slot):
        z_copies[d, unit, slot].wait_recv()
        return zrecv[d, unit, slot].astype(F32)

    def relay(unit, slot):
        for d in range(2):
            dz = (4 - (slot + 1) // 2) * (1, 7)[d] % 8
            q = d if slot % 2 == 0 else 1 - d
            value = part(unit, dz, q)
            if slot > 1:
                value = value + z_got(d, unit, slot - 2)
            z_send(d, unit, slot, value)

    def final(unit, q):
        return part(unit, 0, q) + z_got(q, unit, 6) + z_got(1 - q, unit, 5)

    xb_copies = {}

    def xb_send(dz):
        xb_from[dz] = own[dz, 0, pl.ds(32, 32), :].astype(BF16)
        xb_copies[dz] = send(xb_from.at[dz], xb_recv.at[dz], xb_s.at[dz], xb_r.at[dz], far)

    def xb_wait(*steps):
        for dz in steps:
            xb_copies[dz].wait_recv()

    others(4)
    others(3)
    others(5)
    pl.semaphore_wait(barrier, len(near) + 2)
    for peer in near:
        pl.semaphore_signal(tokens, inc=1, device_id=peer, device_id_type=MESH)
    c0 = send(cgb.at[1 - core], c0buf, c0_s, c0_r, partner)
    for dz in (4, 3, 5):
        send_others(dz)
    for dz in ORDER[3:]:
        others(dz)
        send_others(dz)

    c0.wait_recv()
    cand[...] = jnp.where(root_core == core, cgb[core], c0buf[...])
    cx = send(cand.at[1 - h], cxbuf, cx_s, cx_r, far)

    for dz in (4, 3, 5):
        mine(dz)
        xb_send(dz)
    for unit in range(2):
        relay(unit, 0)
        relay(unit, 1)

    for dz in ORDER[3:]:
        mine(dz)
        xb_send(dz)

    loads[7].wait()
    loads[8].wait()
    wt = (pd[...].astype(F32) * coulomb[...].reshape(1, 512).astype(F32)).astype(BF16)
    r0, p0 = iota((256, 256), 0), iota((256, 256), 1)
    order = one_hot(p0 == (r0 % 8) * 32 + ((r0 // 8) % 8) * 4 + r0 // 64)
    wperm[...] = jnp.dot(order, wt, preferred_element_type=F32).astype(BF16)
    kp = pairs[pl.ds(row, 1), :]
    kc = kp % 32
    target = (kc % 4) * 64 + (kc // 4) * 8 + kp // 32
    perm[...] = one_hot((r0 == target) & (p0 < counts[row]))
    i0 = iota((128, 256), 0)
    for j in range(4):
        pick[j] = one_hot((i0 // 32 == j) & (i0 % 32 == cp % 32))

    relay(0, 2)
    relay(1, 2)
    relay(0, 3)
    relay(1, 3)

    pl.semaphore_wait(tokens, len(near))
    cx.wait_recv()
    quarter[...] = jnp.where(root_h == h, cand[h], cxbuf[...])
    c1 = []
    for i, dz in enumerate(ORDER[:7]):
        zz = (z + dz) % 8
        c1.append(send(quarter.at[zz], c1buf.at[z], c1_s.at[i], c1_r.at[i], at(h, zz, core)))
    c1buf[z] = quarter[z]

    xb_wait(4, 3, 5)
    relay(2, 0)
    relay(2, 1)

    relay(0, 4)
    relay(1, 4)
    relay(0, 5)
    relay(1, 5)

    relay(2, 2)
    xb_wait(2, 6)
    relay(2, 3)

    relay(0, 6)
    relay(1, 6)

    for copy in c1:
        copy.wait_recv()
    colbuf[h, core, z] = c1buf[root_z]
    c2 = []
    for i, (dh, dz) in enumerate(chips):
        slot = colbuf.at[h, core, z]
        c2.append(send(slot, slot, c2_s.at[i], c2_r.at[i], at((h + dh) % 2, (z + dz) % 8, core)))
    c3 = [send(colbuf.at[h, core, z], colbuf.at[h, core, z], c3_s.at[15], c3_r.at[15], partner)]

    relay(2, 4)
    xb_wait(1, 7)
    relay(2, 5)

    for q in range(2):
        xsend[q] = final(0, q).astype(BF16)
    x_copy = send(xsend, xrecv, x_s, x_r, far)
    for q in range(2):
        mine_sum[pl.ds(q * 16, 16), :] = final(1, q)
    relay(2, 6)
    xb_wait(0)
    for q in range(2):
        mine_sum[pl.ds(32 + q * 16, 16), :] = final(2, q)

    loads[6].wait()
    x_copy.wait_recv()
    sv = jnp.concatenate(
        [mine_sum[0:32, :] + xrecv[...].reshape(32, 512).astype(F32), mine_sum[32:64, :]], axis=0
    ).astype(BF16)
    w0, w1 = iota((64, 64), 0), iota((64, 64), 1)
    swap = one_hot(w1 == (w0 % 8) * 8 + w0 // 8)
    sv = jnp.dot(swap, sv, preferred_element_type=F32).astype(BF16)
    dt = dot_t(sv, cond[...]).astype(BF16)
    dt = jnp.concatenate([dt[:, b * 128 : b * 128 + 128] for b in range(8)], axis=0)
    v_of = cp // 32
    for j in range(4):
        e = jnp.dot(dt, pick[j], preferred_element_type=F32).reshape(8, 8, 8, 256)
        total = jnp.where(v_of == 0, e[:, 0], 0.0)
        for v in range(1, 8):
            total = total + jnp.where(v_of == v, e[:, v], 0.0)
        direct[j] = total.reshape(64, 256)

    for i in reversed(range(15)):
        dh, dz = chips[i]
        c2[i].wait_recv()
        slot = colbuf.at[(h + dh) % 2, core, (z + 8 - dz) % 8]
        c3.append(send(slot, slot, c3_s.at[i], c3_r.at[i], partner))
    for copy in c3:
        copy.wait_recv()
    exch = 2.0 * (
        dot_t(wperm[:, 0:256], colbuf[0].reshape(256, 256))
        + dot_t(wperm[:, 256:512], colbuf[1].reshape(256, 256))
    )
    parts = [exch[j * 64 : j * 64 + 64, :] - direct[j] for j in range(4)]
    for d in range(8):
        piece = jnp.concatenate([p[:, d * 32 : d * 32 + 32] for p in parts], axis=1)
        gsend[d] = piece.astype(BF16)
    g_copies = []
    for d in range(1, 8):
        to = (ga + d) % 8
        g_copies.append(
            send(gsend.at[to], grecv.at[d - 1], g_s.at[d - 1], g_r.at[d - 1], {"row": row, "ga": to})
        )
    total = gsend[ga].astype(F32)
    for d, copy in enumerate(g_copies):
        copy.wait_recv()
        total = total + grecv[d].astype(F32)
    total = total.astype(BF16).astype(F32)
    stacked = jnp.concatenate(
        [total if j == 0 else pltpu.roll(total, 128 - 32 * j, 1) for j in range(4)], axis=0
    ).astype(BF16)
    result = dot_l(stacked, perm[...])[0:32]
    slot = ga * 32 + iota((32, 256), 0)
    out_ref[...] = jnp.where(slot < counts[ck], result, 0.0).astype(BF16)
    for copy in sent:
        copy.wait_send()


def per_device(
    pair_dens, cond_dens, val_dens, screened, coulomb, pair_list, counts, q_index, column_k
):
    dma = pltpu.SemaphoreType.DMA
    vmem = pl.BlockSpec(memory_space=pltpu.VMEM)
    hbm = pl.BlockSpec(memory_space=pltpu.HBM)
    return pl.pallas_call(
        kernel,
        out_shape=jax.ShapeDtypeStruct((32, 256), BF16),
        in_specs=[hbm] * 9,
        out_specs=vmem,
        scratch_shapes=[
            pltpu.SMEM((32,), jnp.int32),
            pltpu.SMEM((32,), jnp.int32),
            pltpu.SMEM((1,), jnp.int32),
            pltpu.VMEM((32, 256), jnp.int32),
            pltpu.VMEM((512,), BF16),
            pltpu.VMEM((256, 512), BF16),
            pltpu.VMEM((1024, 512), BF16),
            pltpu.VMEM((32, 64, 128), BF16),
            pltpu.VMEM((8, 512, 128), BF16),
            pltpu.VMEM((8, 2, 64, 512), F32),
            pltpu.VMEM((8, 2, 64, 512), BF16),
            pltpu.VMEM((8, 2, 64, 512), BF16),
            pltpu.VMEM((2, 3, 7, 16, 512), BF16),
            pltpu.VMEM((2, 3, 7, 16, 512), BF16),
            pltpu.VMEM((8, 32, 512), BF16),
            pltpu.VMEM((8, 32, 512), BF16),
            pltpu.VMEM((2, 16, 512), BF16),
            pltpu.VMEM((2, 16, 512), BF16),
            pltpu.VMEM((64, 512), F32),
            pltpu.VMEM((2, 2, 8, 16, 256), BF16),
            pltpu.VMEM((2, 8, 16, 256), BF16),
            pltpu.VMEM((2, 8, 16, 256), BF16),
            pltpu.VMEM((8, 16, 256), BF16),
            pltpu.VMEM((8, 16, 256), BF16),
            pltpu.VMEM((8, 16, 256), BF16),
            pltpu.VMEM((2, 2, 8, 16, 256), BF16),
            pltpu.VMEM((256, 256), BF16),
            pltpu.VMEM((256, 512), BF16),
            pltpu.VMEM((4, 128, 256), BF16),
            pltpu.VMEM((4, 64, 256), F32),
            pltpu.VMEM((8, 64, 128), BF16),
            pltpu.VMEM((7, 64, 128), BF16),
            dma((9,)),
            dma((8,)), dma((8,)),
            dma((2, 3, 7)), dma((2, 3, 7)),
            dma((8,)), dma((8,)),
            dma, dma,
            dma, dma,
            dma, dma,
            dma((7,)), dma((7,)),
            dma((15,)), dma((15,)),
            dma((16,)), dma((16,)),
            dma((7,)), dma((7,)),
            pltpu.SemaphoreType.REGULAR,
        ],
        compiler_params=pltpu.CompilerParams(
            collective_id=0, has_side_effects=True, vmem_limit_bytes=56524800
        ),
        name="bse_block",
    )(
        counts, q_index, column_k, pair_list, coulomb,
        pair_dens, cond_dens, val_dens, screened,
    ).T


def solution(mesh):
    placed = (
        P("row", None, "ga"),
        P("row", None, "ga"),
        P(None, None, "row"),
        P(None, "ga", "row"),
        P("ga"),
        P(),
        P(),
        P(),
        P(),
    )
    return jax.shard_map(
        per_device, mesh=mesh, in_specs=placed, out_specs=P("row", "ga"), check_vma=False
    )
```
